128 devices in a mesh: stn: 32 (over z_hi, y, x), pts: 2 (over core), freq: 2 (over z_lo).
Axes of the slice: x: 4, y: 4, z: 4 (z_hi: 2, z_lo: 2; z = z_hi * 2 + z_lo), core: 2. Of those that a mesh axis runs over, the one named last changes fastest.
Arguments:
- greens: bfloat16 [2, 4, 2048, 4096], P(None, 'freq', 'stn', 'pts'), may hold values from -6 to 6
- noise_weights: bfloat16 [2, 4, 2048, 2048], P(None, 'freq', 'stn'), may hold values from -12 to 12, as said below
Outputs:
- kernel: float32 [4096], P('pts')
The draws below stay inside these ranges and needn't reach their ends.
Inputs may be any that keep to these rules, and one draw needn't show every extreme that they name: For every frequency, noise_weights[0] is symmetric and noise_weights[1] antisymmetric in the two station dimensions, so each frequency's matrix is Hermitian.
All inputs are finite; a program needn't handle non-finite values. Where the reference program divides by a largest or mean magnitude, that divisor is 1e-20 or more.
Results may differ from the reference program's by a relative error of at most 0.0003.
Values may be sent and summed in bfloat16 or wider, within the bound.
A program may use at most 192 MiB of HBM per device.

```python
import jax
import jax.numpy as jnp
from jax import lax

S = 2048
F = 4
P_SIZE = 4096


def draw_noise_weights(key, part):
    base = jax.random.fold_in(key, 11)
    key_real, key_imag = jax.random.split(base, 2)
    rough_real = jax.random.truncated_normal(key_real, -4.0, 4.0, (F, S, S), jnp.float32) * 0.5
    rough_imag = jax.random.truncated_normal(key_imag, -4.0, 4.0, (F, S, S), jnp.float32) * 0.5
    symmetric = (rough_real + jnp.swapaxes(rough_real, 1, 2)) * 0.7071
    antisymmetric = (rough_imag - jnp.swapaxes(rough_imag, 1, 2)) * 0.7071
    return jnp.stack([symmetric, antisymmetric]).astype(jnp.bfloat16)


def levels(own_key, shape, shards, least, high):
    def one(position, blocks):
        steps = jax.random.uniform(jax.random.fold_in(jax.random.fold_in(own_key, 6), position), (blocks,), jnp.float32, least / len(shards), high / len(shards))
        return jnp.repeat(jnp.exp(steps), shape[position] // blocks).reshape((-1,) + (1,) * (len(shape) - position - 1))

    factor_of = one(*shards[0])
    for cut in shards[1:]:
        factor_of = factor_of * one(*cut)
    return factor_of


def noise(key, dims, deviation, most, pieces=(), kind=jnp.bfloat16):
    level = levels(key, dims, pieces, -0.22, 0.18) if pieces else 1.0
    result = jax.random.normal(key, dims, jnp.float32) * deviation * level
    return jnp.minimum(jnp.maximum(result, -most), most).astype(kind)


def setup_inputs(seed: int = 0) -> dict:
    seeds = jax.random.split(jax.random.key(seed), 3)
    greens = noise(seeds[0], (2, F, S, P_SIZE), 1.0, 6.0, ((1, 2), (2, 32), (3, 2)))
    noise_weights = draw_noise_weights(jax.random.fold_in(seeds[2], 71), 0)
    return {"greens": greens, "noise_weights": noise_weights}


def per_frequency(operands):
    green_block, weight_block = operands
    product_real = jnp.dot(weight_block[0], green_block[0], preferred_element_type=jnp.float32) - jnp.dot(weight_block[1], green_block[1], preferred_element_type=jnp.float32)
    product_imag = jnp.dot(weight_block[0], green_block[1], preferred_element_type=jnp.float32) + jnp.dot(weight_block[1], green_block[0], preferred_element_type=jnp.float32)
    green_real = green_block[0].astype(jnp.float32)
    green_imag = green_block[1].astype(jnp.float32)
    return jnp.sum(green_real * product_real + green_imag * product_imag, axis=0)


def reference(greens, noise_weights):
    stacked = lax.map(per_frequency, (jnp.moveaxis(greens, 1, 0), jnp.moveaxis(noise_weights, 1, 0)))
    raw_kernel = jnp.sum(stacked, axis=0) / S
    largest = jnp.max(jnp.abs(raw_kernel))
    return raw_kernel / (largest + 1e-6)
```

```python
import jax
import jax.numpy as jnp
from jax import lax
from jax.experimental import pallas as pl
from jax.experimental.pallas import tpu as pltpu
from jax.sharding import PartitionSpec as P

MESH = pl.DeviceIdType.MESH
SIDE = 4
RUN = 64
BLOCK = 512
POINTS = 512
HALF = 256

SPREAD = [(dx, 0, dz, 0) for dx in (0, 1, 3, 2) for dz in (1, 3)]
PLANE = [(0, dy, dz, 0) for dz in range(SIDE) for dy in range(SIDE) if dy or dz]
ROW = [(dx, 0, 0, dc) for dx in range(SIDE) for dc in range(2) if dx or dc]
PARTNERS = list(dict.fromkeys(SPREAD + PLANE + ROW))


def place():
    stn = lax.axis_index("stn")
    x, y = stn % SIDE, stn // SIDE % SIDE
    z = stn // (SIDE * SIDE) * 2 + lax.axis_index("freq")
    return x, y, z, lax.axis_index("pts")


def device(here, dx=0, dy=0, dz=0, dc=0):
    x, y, z, core = here
    x, y, z, core = (x + dx) % SIDE, (y + dy) % SIDE, (z + dz) % SIDE, (core + dc) % 2
    return {"stn": z // 2 * (SIDE * SIDE) + y * SIDE + x, "freq": z % 2, "pts": core}


def at_multiple(index, size, length):
    return pl.ds(pl.multiple_of(index * size, size), length)


def kernel(
    greens,
    weights,
    out,
    own,
    near,
    far,
    transit,
    mix,
    parts,
    total,
    sums,
    g_send,
    g_recv,
    near_send,
    near_recv,
    hop_send,
    hop_recv,
    far_send,
    far_recv,
    wz_send,
    wz_recv,
    wx_send,
    wx_recv,
    wt_send,
    wt_recv,
    sum_send,
    sum_recv,
    row_send,
    row_recv,
):
    here = place()
    x, y, z, core = here

    barrier = pltpu.get_barrier_semaphore()
    for step in PARTNERS:
        pl.semaphore_signal(barrier, inc=1, device_id=device(here, *step), device_id_type=MESH)
    pl.semaphore_wait(barrier, len(PARTNERS))

    sent = []

    def send(src, dst, send_sem, recv_sem, step):
        copy = pltpu.make_async_remote_copy(
            src_ref=src,
            dst_ref=dst,
            send_sem=send_sem,
            recv_sem=recv_sem,
            device_id=device(here, *step),
            device_id_type=MESH,
        )
        copy.start()
        sent.append(copy)

    def arrived(dst, sem):
        pltpu.make_async_remote_copy(
            src_ref=dst,
            dst_ref=dst,
            send_sem=sem,
            recv_sem=sem,
            device_id=device(here, 1),
            device_id_type=MESH,
        ).wait_recv()

    def rank(dx, dz):
        return (z + dz) % SIDE // 2 * SIDE + (x + dx) % SIDE

    def rows(index):
        return at_multiple(index, RUN, RUN)

    mine = rank(0, 0)
    half = at_multiple(core, HALF, HALF)

    def send_greens(dx, dz):
        kept = (z + dz) % SIDE // 2
        send(
            greens.at[:, kept, :, at_multiple((x + dx) % SIDE, POINTS, POINTS)],
            own.at[:, rows(mine), :],
            g_send.at[SPREAD.index((dx, 0, dz, 0))],
            g_recv.at[mine],
            (dx, 0, dz),
        )

    def send_weights(dz):
        kept = (z + dz) % SIDE // 2
        for d in range(3):
            send(
                weights.at[:, kept, :, at_multiple(core * SIDE + (y + d) % SIDE, HALF, HALF)],
                mix.at[:, d, rows(mine), half],
                wz_send.at[dz // 2, d],
                wz_recv.at[z // 2, d],
                (0, 0, dz),
            )

    for dz in (1, 3):
        send_greens(0, dz)
    for dz in (1, 3):
        send_weights(dz)
    for dx in (1, 3, 2):
        for dz in (1, 3):
            send_greens(dx, dz)

    def mix_at(index):
        return mix.at[:, :, rows(index), half]

    def to_twin(index, slot):
        send(mix_at(index), mix_at(index), wt_send.at[slot], wt_recv.at[index], (0, 0, 0, 1))

    def green_piece(dx, dz):
        index = rank(dx, dz)
        slot = SPREAD.index((dx, 0, dz, 0))
        piece = own.at[:, rows(index), :]
        arrived(piece, g_recv.at[index])
        send(piece, near.at[:, rows(index), :], near_send.at[slot], near_recv.at[index], (0, 3, 0))
        other = at_multiple((y + 2) % SIDE // 2, HALF, HALF)
        send(
            own.at[:, rows(index), other],
            transit.at[:, rows(index), :],
            hop_send.at[slot],
            hop_recv.at[index],
            (0, 1, 0),
        )

    def pass_on(dx, dz):
        index = rank(dx, dz)
        slot = SPREAD.index((dx, 0, dz, 0))
        piece = transit.at[:, rows(index), :]
        arrived(piece, hop_recv.at[index])
        send(piece, far.at[:, rows(index), :], far_send.at[slot], far_recv.at[index], (0, 1, 0))

    for dz in (1, 3):
        green_piece(0, dz)
    for dz in (1, 3):
        zs = (z + dz) % SIDE // 2
        for d in range(3):
            arrived(mix.at[:, d, rows(rank(0, dz)), half], wz_recv.at[zs, d])
        index = rank(0, dz)
        for k, dx in enumerate((1, 3)):
            send(mix_at(index), mix_at(index), wx_send.at[k, dz // 2], wx_recv.at[index], (dx, 0, 0))
        to_twin(index, dz // 2)
    for dx in (1, 3):
        for dz in (1, 3):
            green_piece(dx, dz)
    for dz in (1, 3):
        pass_on(0, dz)
    for k, dx in enumerate((1, 3)):
        for zs in range(2):
            index = zs * SIDE + (x + dx) % SIDE
            arrived(mix_at(index), wx_recv.at[index])
            if zs == k:
                send(mix_at(index), mix_at(index), wx_send.at[2, k], wx_recv.at[index], (-dx % SIDE, 0, 0))
            to_twin(index, 2 + k * 2 + zs)
    for dz in (1, 3):
        green_piece(2, dz)
    for dx in (1, 3, 2):
        for dz in (1, 3):
            pass_on(dx, dz)
    for zs in range(2):
        index = zs * SIDE + (x + 2) % SIDE
        arrived(mix_at(index), wx_recv.at[index])
        to_twin(index, 6 + zs)
    for index in range(2 * SIDE):
        arrived(mix.at[:, :, rows(index), at_multiple(1 - core, HALF, HALF)], wt_recv.at[index])

    total[...] = jnp.zeros_like(total)

    def add_block(d, others, at_others, at_own, columns, weight):
        gr, gi = others[0, :, at_others], others[1, :, at_others]
        partial = jnp.zeros((8, HALF), jnp.float32)
        for m in range(0, BLOCK, HALF):
            wr, wi = mix[0, d, m : m + HALF, :], mix[1, d, m : m + HALF, :]

            def dot(a, b):
                return jnp.dot(a, b, preferred_element_type=jnp.float32)

            re = dot(wr, gr) - dot(wi, gi)
            im = dot(wr, gi) + dot(wi, gr)
            a = own[0, m : m + HALF, at_own].astype(jnp.float32)
            b = own[1, m : m + HALF, at_own].astype(jnp.float32)
            partial = partial + jnp.sum((a * re + b * im).reshape(HALF // 8, 8, HALF), axis=0)
        total[:, columns] += weight * partial

    for n in range(0, POINTS, HALF):
        span = slice(n, n + HALF)
        add_block(0, own, span, span, span, 1.0)
    for index in range(2 * SIDE):
        arrived(near.at[:, rows(index), :], near_recv.at[index])
    for n in range(0, POINTS, HALF):
        span = slice(n, n + HALF)
        add_block(1, near, span, span, span, 2.0)
    for index in range(2 * SIDE):
        arrived(far.at[:, rows(index), :], far_recv.at[index])
    here_half = at_multiple(y // 2, HALF, HALF)
    add_block(2, far, slice(0, HALF), here_half, here_half, 2.0)

    place_in_plane = z * SIDE + y
    stations = 2 * SIDE * SIDE * RUN
    parts[place_in_plane] = jnp.sum(total[...], axis=0, keepdims=True) / stations
    for k, step in enumerate(PLANE):
        mine_part = parts.at[place_in_plane]
        send(mine_part, mine_part, sum_send.at[k], sum_recv.at[place_in_plane], step)
    for _, dy, dz, _ in PLANE:
        slot = (z + dz) % SIDE * SIDE + (y + dy) % SIDE
        arrived(parts.at[slot], sum_recv.at[slot])
    raw = parts[0]
    for slot in range(1, SIDE * SIDE):
        raw = raw + parts[slot]
    place_in_row = core * SIDE + x
    sums[place_in_row] = raw
    for k, step in enumerate(ROW):
        mine_sum = sums.at[place_in_row]
        send(mine_sum, mine_sum, row_send.at[k], row_recv.at[place_in_row], step)
    for dx, _, _, dc in ROW:
        slot = (core + dc) % 2 * SIDE + (x + dx) % SIDE
        arrived(sums.at[slot], row_recv.at[slot])
    largest = jnp.max(jnp.abs(sums[...]))
    for k in range(SIDE):
        out[k] = sums[core * SIDE + k] / (largest + 1e-06)
    for copy in sent:
        copy.wait_send()


def body(greens, noise_weights):
    dma = pltpu.SemaphoreType.DMA
    spread, plane, row = len(SPREAD), len(PLANE), len(ROW)
    ranks = 2 * SIDE
    kernel_of_points = pl.pallas_call(
        kernel,
        out_shape=jax.ShapeDtypeStruct((SIDE, 1, POINTS), jnp.float32),
        in_specs=[pl.BlockSpec(memory_space=pl.ANY)] * 2,
        out_specs=pl.BlockSpec(memory_space=pltpu.VMEM),
        scratch_shapes=[
            pltpu.VMEM((2, BLOCK, POINTS), jnp.bfloat16),
            pltpu.VMEM((2, BLOCK, POINTS), jnp.bfloat16),
            pltpu.VMEM((2, BLOCK, HALF), jnp.bfloat16),
            pltpu.VMEM((2, BLOCK, HALF), jnp.bfloat16),
            pltpu.VMEM((2, 3, BLOCK, BLOCK), jnp.bfloat16),
            pltpu.VMEM((SIDE * SIDE, 1, POINTS), jnp.float32),
            pltpu.VMEM((8, POINTS), jnp.float32),
            pltpu.VMEM((ranks, 1, POINTS), jnp.float32),
            dma((spread,)),
            dma((ranks,)),
            dma((spread,)),
            dma((ranks,)),
            dma((spread,)),
            dma((ranks,)),
            dma((spread,)),
            dma((ranks,)),
            dma((2, 3)),
            dma((2, 3)),
            dma((3, 2)),
            dma((ranks,)),
            dma((ranks,)),
            dma((ranks,)),
            dma((plane,)),
            dma((plane + 1,)),
            dma((row,)),
            dma((row + 1,)),
        ],
        compiler_params=pltpu.CompilerParams(
            collective_id=0, has_side_effects=True, vmem_limit_bytes=48 * 2**20
        ),
    )(greens, noise_weights)
    return kernel_of_points.reshape(SIDE * POINTS)


def solution(mesh):
    in_specs = (P(None, "freq", "stn", "pts"), P(None, "freq", "stn", None))
    out_specs = P("pts")
    return jax.shard_map(body, mesh=mesh, in_specs=in_specs, out_specs=out_specs, check_vma=False)
```

```python
import jax
import jax.numpy as jnp
from jax import lax
from jax.experimental import pallas as pl
from jax.experimental.pallas import tpu as pltpu
from jax.sharding import PartitionSpec as P

MESH = pl.DeviceIdType.MESH
SIDE = 4
RUN = 64
BLOCK = 512
POINTS = 512
HALF = 256

SPREAD = [(dx, 0, dz, 0) for dx in (0, 1, 3, 2) for dz in (1, 3)]
PLANE = [(0, dy, dz, 0) for dz in range(SIDE) for dy in range(SIDE) if dy or dz]
ROW = [(dx, 0, 0, dc) for dx in range(SIDE) for dc in range(2) if dx or dc]
OUTGOING = [(0, 1), (0, 3), (1, 3), (3, 3), (1, 1), (3, 1), (2, 3), (2, 1)]
NEAREST = [(1, 0, 0), (3, 0, 0), (2, 0, 0), (0, 1, 0), (0, 3, 0), (0, 0, 1), (0, 0, 3), (0, 0, 0, 1)]


def place():
    stn = lax.axis_index("stn")
    x, y = stn % SIDE, stn // SIDE % SIDE
    z = stn // (SIDE * SIDE) * 2 + lax.axis_index("freq")
    return x, y, z, lax.axis_index("pts")


def device(here, dx=0, dy=0, dz=0, dc=0):
    x, y, z, core = here
    x, y, z, core = (x + dx) % SIDE, (y + dy) % SIDE, (z + dz) % SIDE, (core + dc) % 2
    return {"stn": z // 2 * (SIDE * SIDE) + y * SIDE + x, "freq": z % 2, "pts": core}


def at_multiple(index, size, length):
    return pl.ds(pl.multiple_of(index * size, size), length)


def kernel(
    greens,
    weights,
    out,
    own,
    near,
    far,
    transit,
    mix,
    parts,
    total,
    sums,
    g_send,
    g_recv,
    near_send,
    near_recv,
    hop_send,
    hop_recv,
    far_send,
    far_recv,
    wz_send,
    wz_recv,
    wx_send,
    wx_recv,
    wt_send,
    wt_recv,
    sum_send,
    sum_recv,
    row_send,
    row_recv,
    greens_here,
    weights_here,
    load,
    stage_x,
    stage_z,
    stage_recv,
    forward_send,
):
    here = place()
    x, y, z, core = here

    barrier = pltpu.get_barrier_semaphore()
    for step in NEAREST:
        pl.semaphore_signal(barrier, inc=1, device_id=device(here, *step), device_id_type=MESH)

    def at_greens(dx, dz):
        columns = at_multiple((x + dx) % SIDE, POINTS, POINTS)
        return slice(None), (z + dz) % SIDE // 2, slice(None), columns

    greens_in = {}
    for k, (dx, dz) in enumerate(OUTGOING):
        part = at_greens(dx, dz)
        greens_in[dx, dz] = pltpu.make_async_copy(greens.at[part], greens_here.at[k], load.at[k])
        greens_in[dx, dz].start()
    for d in range(3):
        columns = at_multiple(core * SIDE + (y + d) % SIDE, HALF, HALF)
        pltpu.make_async_copy(
            weights.at[:, :, :, columns], weights_here.at[:, :, d], load.at[len(OUTGOING)]
        ).start()
    pl.semaphore_wait(barrier, len(NEAREST))

    def send(src, dst, send_sem, recv_sem, step):
        copy = pltpu.make_async_remote_copy(
            src_ref=src,
            dst_ref=dst,
            send_sem=send_sem,
            recv_sem=recv_sem,
            device_id=device(here, *step),
            device_id_type=MESH,
        )
        copy.start()

    def arrived(dst, sem):
        pltpu.make_async_remote_copy(
            src_ref=dst,
            dst_ref=dst,
            send_sem=sem,
            recv_sem=sem,
            device_id=device(here, 1),
            device_id_type=MESH,
        ).wait_recv()

    def left(src, sem):
        pltpu.make_async_remote_copy(
            src_ref=src,
            dst_ref=src,
            send_sem=sem,
            recv_sem=sem,
            device_id=device(here, 1),
            device_id_type=MESH,
        ).wait_send()

    def rank(dx, dz):
        return (z + dz) % SIDE // 2 * SIDE + (x + dx) % SIDE

    def rows(index):
        return at_multiple(index, RUN, RUN)

    mine = rank(0, 0)
    half = at_multiple(core, HALF, HALF)

    def send_greens(dx, dz):
        piece = greens_here.at[OUTGOING.index((dx, dz))]
        greens_in[dx, dz].wait()
        if dx == 0:
            send(piece, own.at[:, rows(mine), :], g_send, g_recv.at[mine], (0, 0, dz))
        elif dz == 1:
            send(piece, stage_z.at[dx - 1], g_send, stage_recv.at[0, dx - 1], (0, 0, dz))
        else:
            send(piece, stage_x.at[dx - 1], g_send, stage_recv.at[1, dx - 1], (dx, 0, 0))

    def forward_x(dx):
        piece, index = stage_z.at[dx - 1], rank(0, 3)
        arrived(piece, stage_recv.at[0, dx - 1])
        send(piece, own.at[:, rows(index), :], forward_send, g_recv.at[index], (dx, 0, 0))

    def forward_z(dx):
        piece, index = stage_x.at[dx - 1], rank(-dx, 0)
        arrived(piece, stage_recv.at[1, dx - 1])
        send(piece, own.at[:, rows(index), :], forward_send, g_recv.at[index], (0, 0, 3))

    def send_weights(dz, d):
        kept = (z + dz) % SIDE // 2
        send(
            weights_here.at[:, kept, d],
            mix_at(mine, d),
            wz_send,
            wz_recv.at[z // 2, d],
            (0, 0, dz),
        )

    def mix_at(index, d):
        return mix.at[:, d, rows(index), half]

    def to_twin(index, d, dz):
        piece = mix_at(index, d)
        send(piece, piece, wt_send, wt_recv.at[dz // 2, d], (0, 0, 0, 1))

    def green_piece(dx, dz):
        index = rank(dx, dz)
        piece = own.at[:, rows(index), :]
        arrived(piece, g_recv.at[index])
        send(piece, near.at[:, rows(index), :], near_send, near_recv, (0, 3, 0))
        other = at_multiple((y + 2) % SIDE // 2, HALF, HALF)
        send(
            own.at[:, rows(index), other],
            transit.at[:, rows(index), :],
            hop_send,
            hop_recv.at[index],
            (0, 1, 0),
        )

    def pass_on(dx, dz):
        index = rank(dx, dz)
        piece = transit.at[:, rows(index), :]
        arrived(piece, hop_recv.at[index])
        send(piece, far.at[:, rows(index), :], far_send, far_recv, (0, 1, 0))

    def weights_along_z(d, dz):
        index = rank(0, dz)
        piece = mix_at(index, d)
        arrived(piece, wz_recv.at[(z + dz) % SIDE // 2, d])
        for dx in (1, 3):
            send(piece, piece, wx_send, wx_recv.at[SIDE - dx - 1, dz // 2, d], (dx, 0, 0))
        to_twin(index, d, dz)

    def weights_along_x(d, dz):
        for k, dx in enumerate((1, 3)):
            index = rank(dx, dz)
            piece = mix_at(index, d)
            arrived(piece, wx_recv.at[dx - 1, dz // 2, d])
            if dz // 2 == k:
                send(piece, piece, wx_send, wx_recv.at[1, dz // 2, d], (-dx % SIDE, 0, 0))
            to_twin(index, d, dz)

    def weights_across(d, dz):
        index = rank(2, dz)
        arrived(mix_at(index, d), wx_recv.at[1, dz // 2, d])
        to_twin(index, d, dz)

    def weights_from_twin(d, dz):
        part = at_multiple((z + dz) % SIDE // 2, HALF, HALF)
        arrived(mix.at[:, d, part, at_multiple(1 - core, HALF, HALF)], wt_recv.at[dz // 2, d])

    total[...] = jnp.zeros_like(total)

    def add_block(d, dz, others, at_others, at_own, columns, weight):
        gr, gi = others[0, :, at_others], others[1, :, at_others]
        part = at_multiple((z + dz) % SIDE // 2, HALF, HALF)
        wr, wi = mix[0, d, part, :], mix[1, d, part, :]

        def dot(a, b):
            return jnp.dot(a, b, preferred_element_type=jnp.float32)

        re = dot(wr, gr) - dot(wi, gi)
        im = dot(wr, gi) + dot(wi, gr)
        a = own[0, part, at_own].astype(jnp.float32)
        b = own[1, part, at_own].astype(jnp.float32)
        partial = jnp.sum((a * re + b * im).reshape(HALF // 8, 8, HALF), axis=0)
        total[:, columns] += weight * partial

    def add_whole(d, dz, others, weight):
        weights_from_twin(d, dz)
        for n in range(0, POINTS, HALF):
            span = slice(n, n + HALF)
            add_block(d, dz, others, span, span, span, weight)

    for dz in (1, 3):
        send_greens(0, dz)
    for dx in (1, 3, 2):
        send_greens(dx, 3)
    pltpu.make_async_copy(weights_here, weights_here, load.at[len(OUTGOING)]).wait()
    send_weights(3, 0)
    send_greens(1, 1)
    send_weights(3, 1)
    send_greens(3, 1)
    send_weights(3, 2)
    send_greens(2, 1)
    for d in range(3):
        send_weights(1, d)
    green_piece(0, 1)
    green_piece(0, 3)
    forward_z(1)
    forward_z(3)
    weights_along_z(0, 1)
    weights_along_z(1, 1)
    forward_x(1)
    weights_along_z(2, 1)
    pass_on(0, 1)
    forward_z(2)
    pass_on(0, 3)
    forward_x(3)
    green_piece(3, 1)
    weights_along_x(0, 1)
    green_piece(1, 3)
    green_piece(1, 1)
    forward_x(2)
    weights_along_x(1, 1)
    green_piece(3, 3)
    weights_along_z(0, 3)
    weights_along_x(2, 1)
    pass_on(3, 1)
    green_piece(2, 1)
    weights_along_z(1, 3)
    weights_along_z(2, 3)
    weights_across(0, 1)
    green_piece(2, 3)
    pass_on(1, 3)
    weights_across(1, 1)
    pass_on(1, 1)
    pass_on(3, 3)
    weights_across(2, 1)
    weights_along_x(0, 3)
    weights_along_x(1, 3)
    pass_on(2, 1)
    weights_along_x(2, 3)
    add_whole(0, 1, own, 1.0)
    weights_across(0, 3)
    weights_across(1, 3)
    weights_across(2, 3)
    pass_on(2, 3)
    add_whole(0, 3, own, 1.0)
    arrived(near, near_recv)
    add_whole(1, 1, near, 2.0)
    add_whole(1, 3, near, 2.0)
    arrived(far, far_recv)
    here_half = at_multiple(y // 2, HALF, HALF)
    for dz in (1, 3):
        weights_from_twin(2, dz)
        add_block(2, dz, far, slice(0, HALF), here_half, here_half, 2.0)

    place_in_plane = z * SIDE + y
    stations = 2 * SIDE * SIDE * RUN
    parts[place_in_plane] = jnp.sum(total[...], axis=0, keepdims=True) / stations
    for step in PLANE:
        mine_part = parts.at[place_in_plane]
        send(mine_part, mine_part, sum_send, sum_recv, step)
    arrived(parts.at[: len(PLANE)], sum_recv)
    raw = parts[0]
    for slot in range(1, SIDE * SIDE):
        raw = raw + parts[slot]
    place_in_row = core * SIDE + x
    sums[place_in_row] = raw
    for step in ROW:
        mine_sum = sums.at[place_in_row]
        send(mine_sum, mine_sum, row_send, row_recv, step)
    arrived(sums.at[: len(ROW)], row_recv)
    largest = jnp.max(jnp.abs(sums[...]))
    for k in range(SIDE):
        out[k] = sums[core * SIDE + k] / (largest + 1e-06)
    left(own, g_send)
    left(own.at[:, : 6 * RUN, :], forward_send)
    left(own, near_send)
    left(transit, hop_send)
    left(far, far_send)
    left(mix.at[:, :, : 2 * RUN, half], wz_send)
    left(mix.at[:, :, : 6 * RUN, half], wx_send)
    left(mix.at[:, :, :, half], wt_send)
    left(parts.at[: len(PLANE)], sum_send)
    left(sums.at[: len(ROW)], row_send)


def body(greens, noise_weights):
    dma = pltpu.SemaphoreType.DMA
    spread = len(SPREAD)
    ranks = 2 * SIDE
    kernel_of_points = pl.pallas_call(
        kernel,
        out_shape=jax.ShapeDtypeStruct((SIDE, 1, POINTS), jnp.float32),
        in_specs=[pl.BlockSpec(memory_space=pl.ANY)] * 2,
        out_specs=pl.BlockSpec(memory_space=pltpu.VMEM),
        scratch_shapes=[
            pltpu.VMEM((2, BLOCK, POINTS), jnp.bfloat16),
            pltpu.VMEM((2, BLOCK, POINTS), jnp.bfloat16),
            pltpu.VMEM((2, BLOCK, HALF), jnp.bfloat16),
            pltpu.VMEM((2, BLOCK, HALF), jnp.bfloat16),
            pltpu.VMEM((2, 3, BLOCK, BLOCK), jnp.bfloat16),
            pltpu.VMEM((SIDE * SIDE, 1, POINTS), jnp.float32),
            pltpu.VMEM((8, POINTS), jnp.float32),
            pltpu.VMEM((ranks, 1, POINTS), jnp.float32),
            dma,
            dma((ranks,)),
            dma,
            dma,
            dma,
            dma((ranks,)),
            dma,
            dma,
            dma,
            dma((2, 3)),
            dma,
            dma((3, 2, 3)),
            dma,
            dma((2, 3)),
            dma,
            dma,
            dma,
            dma,
            pltpu.VMEM((spread, 2, RUN, POINTS), jnp.bfloat16),
            pltpu.VMEM((2, 2, 3, RUN, HALF), jnp.bfloat16),
            dma((spread + 1,)),
            pltpu.VMEM((3, 2, RUN, POINTS), jnp.bfloat16),
            pltpu.VMEM((3, 2, RUN, POINTS), jnp.bfloat16),
            dma((2, 3)),
            dma,
        ],
        compiler_params=pltpu.CompilerParams(
            collective_id=0, has_side_effects=True, vmem_limit_bytes=213 * 2**18
        ),
    )(greens, noise_weights)
    return kernel_of_points.reshape(SIDE * POINTS)


def solution(mesh):
    in_specs = (P(None, "freq", "stn", "pts"), P(None, "freq", "stn", None))
    out_specs = P("pts")
    return jax.shard_map(body, mesh=mesh, in_specs=in_specs, out_specs=out_specs, check_vma=False)
```

```python
import jax
import jax.numpy as jnp
from jax import lax
from jax.experimental import pallas as pl
from jax.experimental.pallas import tpu as pltpu
from jax.sharding import PartitionSpec as P

MESH = pl.DeviceIdType.MESH
SIDE = 4
RUN = 64
BLOCK = 512
POINTS = 512
HALF = 256

SPREAD = [(dx, 0, dz, 0) for dx in (0, 1, 3, 2) for dz in (1, 3)]
PLANE = [(0, dy, dz, 0) for dz in range(SIDE) for dy in range(SIDE) if dy or dz]
ROW = [(dx, 0, 0, dc) for dx in range(SIDE) for dc in range(2) if dx or dc]
OUTGOING = [(0, 1), (0, 3), (1, 3), (3, 3), (1, 1), (3, 1), (2, 3), (2, 1)]
NEAREST = [(1, 0, 0), (3, 0, 0), (2, 0, 0), (0, 1, 0), (0, 3, 0), (0, 0, 1), (0, 0, 3), (0, 0, 0, 1)]


def place():
    stn = lax.axis_index("stn")
    x, y = stn % SIDE, stn // SIDE % SIDE
    z = stn // (SIDE * SIDE) * 2 + lax.axis_index("freq")
    return x, y, z, lax.axis_index("pts")


def device(here, dx=0, dy=0, dz=0, dc=0):
    x, y, z, core = here
    x, y, z, core = (x + dx) % SIDE, (y + dy) % SIDE, (z + dz) % SIDE, (core + dc) % 2
    return {"stn": z // 2 * (SIDE * SIDE) + y * SIDE + x, "freq": z % 2, "pts": core}


def at_multiple(index, size, length):
    return pl.ds(pl.multiple_of(index * size, size), length)


def kernel(
    greens,
    weights,
    out,
    own,
    near,
    far,
    stage_w,
    mix,
    parts,
    total,
    sums,
    g_send,
    g_recv,
    near_send,
    near_recv,
    wy_send,
    wy_recv,
    far_send,
    far_recv,
    wz_send,
    wz_recv,
    wx_send,
    wx_recv,
    wt_send,
    wt_recv,
    sum_send,
    sum_recv,
    row_send,
    row_recv,
    greens_here,
    weights_here,
    load,
    stage_x,
    stage_z,
    stage_recv,
    forward_send,
    met,
):
    here = place()
    x, y, z, core = here

    barrier = pltpu.get_barrier_semaphore()
    for step in NEAREST:
        pl.semaphore_signal(barrier, inc=1, device_id=device(here, *step), device_id_type=MESH)

    def at_greens(dx, dz):
        columns = at_multiple((x + dx) % SIDE, POINTS, POINTS)
        return slice(None), (z + dz) % SIDE // 2, slice(None), columns

    greens_in = {}
    for k, (dx, dz) in enumerate(OUTGOING):
        part = at_greens(dx, dz)
        greens_in[dx, dz] = pltpu.make_async_copy(greens.at[part], greens_here.at[k], load.at[k])
        greens_in[dx, dz].start()

    brings = pl.when(core == 1)

    @brings
    def load_weights():
        for d in range(3):
            for zs in range(2):
                columns = at_multiple(zs * SIDE + (y + d) % SIDE, HALF, HALF)
                pltpu.make_async_copy(
                    weights.at[:, :, :, columns],
                    weights_here.at[:, :, d, :, zs * HALF : (zs + 1) * HALF],
                    load.at[len(OUTGOING)],
                ).start()

    pl.semaphore_wait(barrier, len(NEAREST))

    def send(src, dst, send_sem, recv_sem, step):
        copy = pltpu.make_async_remote_copy(
            src_ref=src,
            dst_ref=dst,
            send_sem=send_sem,
            recv_sem=recv_sem,
            device_id=device(here, *step),
            device_id_type=MESH,
        )
        copy.start()

    def arrived(dst, sem):
        pltpu.make_async_remote_copy(
            src_ref=dst,
            dst_ref=dst,
            send_sem=sem,
            recv_sem=sem,
            device_id=device(here, 1),
            device_id_type=MESH,
        ).wait_recv()

    def left(src, sem):
        pltpu.make_async_remote_copy(
            src_ref=src,
            dst_ref=src,
            send_sem=sem,
            recv_sem=sem,
            device_id=device(here, 1),
            device_id_type=MESH,
        ).wait_send()

    def rank(dx, dz):
        return (z + dz) % SIDE // 2 * SIDE + (x + dx) % SIDE

    def rows(index):
        return at_multiple(index, RUN, RUN)

    mine = rank(0, 0)

    def half(dz):
        return at_multiple((z + dz) % SIDE // 2, HALF, HALF)

    def send_greens(dx, dz):
        piece = greens_here.at[OUTGOING.index((dx, dz))]
        greens_in[dx, dz].wait()
        if dx == 0:
            send(piece, own.at[:, rows(mine), :], g_send, g_recv.at[mine], (0, 0, dz))
        elif dz == 1:
            send(piece, stage_z.at[dx - 1], g_send, stage_recv.at[0, dx - 1], (0, 0, dz))
        else:
            send(piece, stage_x.at[dx - 1], g_send, stage_recv.at[1, dx - 1], (dx, 0, 0))

    def forward_x(dx):
        piece, index = stage_z.at[dx - 1], rank(0, 3)
        arrived(piece, stage_recv.at[0, dx - 1])
        send(piece, own.at[:, rows(index), :], forward_send, g_recv.at[index], (dx, 0, 0))

    def forward_z(dx):
        piece, index = stage_x.at[dx - 1], rank(-dx, 0)
        arrived(piece, stage_recv.at[1, dx - 1])
        send(piece, own.at[:, rows(index), :], forward_send, g_recv.at[index], (0, 0, 3))

    def send_weights(dz, d):
        kept = (z + dz) % SIDE // 2
        columns = columns_of(d, -dz % SIDE, z // 2)

        @brings
        def to_neighbour():
            send(
                weights_here.at[:, kept, d, :, columns],
                stage_w.at[-dz % SIDE // 2] if d == 2 else mix.at[:, d, rows(mine), columns],
                wz_send,
                wz_recv.at[-dz % SIDE // 2, d],
                (0, 0, dz),
            )

    def columns_of(d, dz, zs):
        return at_multiple(zs, HALF, HALF) if d == 0 and dz == 3 else slice(None)

    def mix_at(index, d, dz):
        return mix.at[:, d, rows(index), columns_of(d, dz, (z + dz) % SIDE // 2)]

    def to_twin(index, d, dz):
        piece = mix_at(index, d, dz)
        send(piece, piece, wt_send.at[d], wt_recv.at[dz // 2, d], (0, 0, 0, 1))

    def green_piece(dx, dz):
        index = rank(dx, dz)
        piece = own.at[:, rows(index), :]
        arrived(piece, g_recv.at[index])
        send(piece, near.at[:, rows(index), :], near_send, near_recv.at[dz // 2], (0, 3, 0))
        other = at_multiple((y + 1) % SIDE // 2, HALF, HALF)
        send(own.at[:, rows(index), other], far.at[:, rows(index), :], far_send, far_recv, (0, 1, 0))

    def spread_weights(index, d, dz):
        piece = mix_at(index, d, dz)
        for dx in (1, 3):
            send(piece, piece, wx_send, wx_recv.at[SIDE - dx - 1, dz // 2, d], (dx, 0, 0))
        to_twin(index, d, dz)

    def weights_along_z(d, dz):
        @brings
        def onward():
            index = rank(0, dz)
            if d == 2:
                piece = stage_w.at[dz // 2]
                arrived(piece, wz_recv.at[dz // 2, d])
                send(piece, mix_at(index, d, dz), wy_send, wy_recv.at[dz // 2], (0, 1, 0))
            else:
                arrived(mix_at(index, d, dz), wz_recv.at[dz // 2, d])
                spread_weights(index, d, dz)

    def weights_along_y(dz):
        @brings
        def onward():
            index = rank(0, dz)
            arrived(mix_at(index, 2, dz), wy_recv.at[dz // 2])
            spread_weights(index, 2, dz)

    def weights_along_x(d, dz):
        @brings
        def spread_out():
            for k, dx in enumerate((1, 3)):
                index = rank(dx, dz)
                piece = mix_at(index, d, dz)
                arrived(piece, wx_recv.at[dx - 1, dz // 2, d])
                if dz // 2 == k:
                    send(piece, piece, wx_send, wx_recv.at[1, dz // 2, d], (-dx % SIDE, 0, 0))
                to_twin(index, d, dz)

    def weights_across(d, dz):
        @brings
        def hand_over():
            index = rank(2, dz)
            arrived(mix_at(index, d, dz), wx_recv.at[1, dz // 2, d])
            to_twin(index, d, dz)

    def weights_from_twin(d, dz):
        @pl.when(core == 0)
        def take():
            columns = columns_of(d, dz, (z + dz) % SIDE // 2)
            arrived(mix.at[:, d, : SIDE * RUN, columns], wt_recv.at[dz // 2, d])

    total[...] = jnp.zeros_like(total)

    def add_block(d, dz, dj, firsts, at_firsts, others, at_others, columns, weight):
        part = half(dz)

        def product(at_j):
            wr, wi = mix[0, d, part, at_j], mix[1, d, part, at_j]
            gr, gi = others[0, at_j, at_others], others[1, at_j, at_others]

            def dot(a, b):
                return jnp.dot(a, b, preferred_element_type=jnp.float32)

            return dot(wr, gr) - dot(wi, gi), dot(wr, gi) + dot(wi, gr)

        if d:
            re, im = product(half(dj))
        else:
            re, im = product(half(dz))
            if dz == 1:
                re2, im2 = product(half(3))
                re, im = re + 2.0 * re2, im + 2.0 * im2
        a = firsts[0, part, at_firsts].astype(jnp.float32)
        b = firsts[1, part, at_firsts].astype(jnp.float32)
        partial = jnp.sum((a * re + b * im).reshape(HALF // 8, 8, HALF), axis=0)
        total[:, columns] += weight * partial

    def add_own(dz):
        weights_from_twin(0, dz)
        for n in range(0, POINTS, HALF):
            span = slice(n, n + HALF)
            add_block(0, dz, None, own, span, own, span, span, 1.0)

    def add_near(dz, dj):
        for n in range(0, POINTS, HALF):
            span = slice(n, n + HALF)
            add_block(1, dz, dj, own, span, near, span, span, 2.0)

    def add_far(dz, dj):
        at_points = at_multiple(y // 2, HALF, HALF)
        add_block(2, dz, dj, far, slice(None), near, at_points, at_points, 2.0)

    for dz in (1, 3):
        send_greens(0, dz)
    for dx in (1, 3, 2):
        send_greens(dx, 3)

    @brings
    def weights_loaded():
        pltpu.make_async_copy(weights_here, weights_here, load.at[len(OUTGOING)]).wait()

    send_weights(3, 0)
    send_greens(1, 1)
    send_weights(1, 2)
    send_greens(3, 1)
    send_weights(1, 0)
    send_weights(1, 1)
    send_greens(2, 1)
    send_weights(3, 2)
    send_weights(3, 1)
    green_piece(0, 1)
    green_piece(0, 3)
    pl.semaphore_signal(met, inc=1, device_id=device(here, 0, 3), device_id_type=MESH)
    forward_z(1)
    forward_z(3)
    weights_along_z(0, 1)
    forward_x(1)
    weights_along_z(2, 1)
    weights_along_z(1, 1)
    forward_z(2)
    forward_x(3)
    green_piece(3, 1)
    weights_along_x(0, 1)
    weights_along_y(1)
    weights_along_z(0, 3)
    green_piece(3, 3)
    weights_along_z(2, 3)
    weights_along_x(1, 1)
    weights_across(0, 1)
    weights_along_z(1, 3)
    green_piece(1, 1)
    weights_along_x(2, 1)
    forward_x(2)
    green_piece(1, 3)
    weights_along_y(3)
    weights_along_x(0, 3)
    weights_across(1, 1)
    green_piece(2, 1)
    weights_across(2, 1)
    weights_along_x(1, 3)
    weights_across(0, 3)
    pl.semaphore_wait(met, 1)
    green_piece(2, 3)
    weights_along_x(2, 3)
    weights_across(1, 3)
    add_own(1)
    add_own(3)
    weights_from_twin(1, 1)
    weights_from_twin(1, 3)
    arrived(near.at[:, half(1), :], near_recv.at[0])
    add_near(1, 1)
    add_near(3, 1)
    weights_from_twin(2, 1)
    arrived(far, far_recv)
    add_far(1, 1)
    arrived(near.at[:, half(3), :], near_recv.at[1])
    add_near(1, 3)
    add_near(3, 3)
    add_far(1, 3)
    weights_across(2, 3)
    weights_from_twin(2, 3)
    add_far(3, 1)
    add_far(3, 3)

    place_in_plane = z * SIDE + y
    stations = 2 * SIDE * SIDE * RUN
    parts[place_in_plane] = jnp.sum(total[...], axis=0, keepdims=True) / stations
    for step in PLANE:
        mine_part = parts.at[place_in_plane]
        send(mine_part, mine_part, sum_send, sum_recv, step)
    arrived(parts.at[: len(PLANE)], sum_recv)
    raw = parts[0]
    for slot in range(1, SIDE * SIDE):
        raw = raw + parts[slot]
    place_in_row = core * SIDE + x
    sums[place_in_row] = raw
    for step in ROW:
        mine_sum = sums.at[place_in_row]
        send(mine_sum, mine_sum, row_send, row_recv, step)
    arrived(sums.at[: len(ROW)], row_recv)
    largest = jnp.max(jnp.abs(sums[...]))
    for k in range(SIDE):
        out[k] = sums[core * SIDE + k] / (largest + 1e-06)
    left(own, g_send)
    left(own.at[:, : 6 * RUN, :], forward_send)
    left(own, near_send)
    left(far, far_send)
    left(parts.at[: len(PLANE)], sum_send)
    left(sums.at[: len(ROW)], row_send)

    @brings
    def weights_left():
        left(mix.at[:, 0, : 11 * RUN // 2, :], wz_send)
        left(mix.at[:, :, : 11 * RUN // 2, :], wx_send)
        left(mix.at[:, 0, : 6 * RUN, :], wt_send.at[0])
        left(mix.at[:, 1], wt_send.at[1])
        left(mix.at[:, 2], wt_send.at[2])
        left(mix.at[:, 0, : 2 * RUN, :], wy_send)


def body(greens, noise_weights):
    dma = pltpu.SemaphoreType.DMA
    spread = len(SPREAD)
    ranks = 2 * SIDE
    kernel_of_points = pl.pallas_call(
        kernel,
        out_shape=jax.ShapeDtypeStruct((SIDE, 1, POINTS), jnp.float32),
        in_specs=[pl.BlockSpec(memory_space=pl.ANY)] * 2,
        out_specs=pl.BlockSpec(memory_space=pltpu.VMEM),
        scratch_shapes=[
            pltpu.VMEM((2, BLOCK, POINTS), jnp.bfloat16),
            pltpu.VMEM((2, BLOCK, POINTS), jnp.bfloat16),
            pltpu.VMEM((2, BLOCK, HALF), jnp.bfloat16),
            pltpu.VMEM((2, 2, RUN, BLOCK), jnp.bfloat16),
            pltpu.VMEM((2, 3, BLOCK, BLOCK), jnp.bfloat16),
            pltpu.VMEM((SIDE * SIDE, 1, POINTS), jnp.float32),
            pltpu.VMEM((8, POINTS), jnp.float32),
            pltpu.VMEM((ranks, 1, POINTS), jnp.float32),
            dma,
            dma((ranks,)),
            dma,
            dma((2,)),
            dma,
            dma((2,)),
            dma,
            dma,
            dma,
            dma((2, 3)),
            dma,
            dma((3, 2, 3)),
            dma((3,)),
            dma((2, 3)),
            dma,
            dma,
            dma,
            dma,
            pltpu.VMEM((spread, 2, RUN, POINTS), jnp.bfloat16),
            pltpu.VMEM((2, 2, 3, RUN, BLOCK), jnp.bfloat16),
            dma((spread + 1,)),
            pltpu.VMEM((3, 2, RUN, POINTS), jnp.bfloat16),
            pltpu.VMEM((3, 2, RUN, POINTS), jnp.bfloat16),
            dma((2, 3)),
            dma,
            pltpu.SemaphoreType.REGULAR,
        ],
        compiler_params=pltpu.CompilerParams(
            collective_id=0, has_side_effects=True, vmem_limit_bytes=213 * 2**18
        ),
    )(greens, noise_weights)
    return kernel_of_points.reshape(SIDE * POINTS)


def solution(mesh):
    in_specs = (P(None, "freq", "stn", "pts"), P(None, "freq", "stn", None))
    out_specs = P("pts")
    return jax.shard_map(body, mesh=mesh, in_specs=in_specs, out_specs=out_specs, check_vma=False)
```

```python
import jax
import jax.numpy as jnp
from jax import lax
from jax.experimental import pallas as pl
from jax.experimental.pallas import tpu as pltpu
from jax.sharding import PartitionSpec as P

MESH = pl.DeviceIdType.MESH
SIDE = 4
RUN = 64
BLOCK = 512
POINTS = 512
HALF = 256

SPREAD = [(dx, 0, dz, 0) for dx in (0, 1, 3, 2) for dz in (1, 3)]
PLANE = [(0, dy, dz, 0) for dz in range(SIDE) for dy in range(SIDE) if dy or dz]
ROW = [(dx, 0, 0, dc) for dx in range(SIDE) for dc in range(2) if dx or dc]
OUTGOING = [(0, 1), (0, 3), (1, 3), (3, 3), (1, 1), (3, 1), (2, 3), (2, 1)]
NEAREST = [(1, 0, 0), (3, 0, 0), (2, 0, 0), (0, 1, 0), (0, 3, 0), (0, 0, 1), (0, 0, 3), (0, 0, 0, 1)]


def place():
    stn = lax.axis_index("stn")
    x, y = stn % SIDE, stn // SIDE % SIDE
    z = stn // (SIDE * SIDE) * 2 + lax.axis_index("freq")
    return x, y, z, lax.axis_index("pts")


def device(here, dx=0, dy=0, dz=0, dc=0):
    x, y, z, core = here
    x, y, z, core = (x + dx) % SIDE, (y + dy) % SIDE, (z + dz) % SIDE, (core + dc) % 2
    return {"stn": z // 2 * (SIDE * SIDE) + y * SIDE + x, "freq": z % 2, "pts": core}


def at_multiple(index, size, length):
    return pl.ds(pl.multiple_of(index * size, size), length)


def kernel(
    greens,
    weights,
    out,
    own,
    near,
    far,
    stage_w,
    mix,
    parts,
    total,
    sums,
    g_send,
    g_recv,
    near_send,
    near_recv,
    wy_send,
    wy_recv,
    far_send,
    far_recv,
    wz_send,
    wz_recv,
    wx_send,
    wx_recv,
    wt_send,
    wt_recv,
    sum_send,
    sum_recv,
    row_send,
    row_recv,
    greens_here,
    weights_here,
    load,
    stage_x,
    stage_z,
    stage_recv,
    forward_send,
    met,
):
    here = place()
    x, y, z, core = here

    barrier = pltpu.get_barrier_semaphore()
    for step in NEAREST:
        pl.semaphore_signal(barrier, inc=1, device_id=device(here, *step), device_id_type=MESH)

    def at_greens(dx, dz):
        columns = at_multiple((x + dx) % SIDE, POINTS, POINTS)
        return slice(None), (z + dz) % SIDE // 2, slice(None), columns

    greens_in = {}
    for k, (dx, dz) in enumerate(OUTGOING):
        part = at_greens(dx, dz)
        greens_in[dx, dz] = pltpu.make_async_copy(greens.at[part], greens_here.at[k], load.at[k])
        greens_in[dx, dz].start()

    brings = pl.when(core == 1)

    @brings
    def load_weights():
        for d in range(3):
            for zs in range(2):
                columns = at_multiple(zs * SIDE + (y + d) % SIDE, HALF, HALF)
                pltpu.make_async_copy(
                    weights.at[:, :, :, columns],
                    weights_here.at[:, :, d, :, zs * HALF : (zs + 1) * HALF],
                    load.at[len(OUTGOING)],
                ).start()

    pl.semaphore_wait(barrier, len(NEAREST))

    def send(src, dst, send_sem, recv_sem, step):
        copy = pltpu.make_async_remote_copy(
            src_ref=src,
            dst_ref=dst,
            send_sem=send_sem,
            recv_sem=recv_sem,
            device_id=device(here, *step),
            device_id_type=MESH,
        )
        copy.start()

    def arrived(dst, sem):
        pltpu.make_async_remote_copy(
            src_ref=dst,
            dst_ref=dst,
            send_sem=sem,
            recv_sem=sem,
            device_id=device(here, 1),
            device_id_type=MESH,
        ).wait_recv()

    def left(src, sem):
        pltpu.make_async_remote_copy(
            src_ref=src,
            dst_ref=src,
            send_sem=sem,
            recv_sem=sem,
            device_id=device(here, 1),
            device_id_type=MESH,
        ).wait_send()

    def rank(dx, dz):
        return (z + dz) % SIDE // 2 * SIDE + (x + dx) % SIDE

    def rows(index):
        return at_multiple(index, RUN, RUN)

    mine = rank(0, 0)

    def half(dz):
        return at_multiple((z + dz) % SIDE // 2, HALF, HALF)

    def send_greens(dx, dz):
        piece = greens_here.at[OUTGOING.index((dx, dz))]
        greens_in[dx, dz].wait()
        for c in range(2):
            if dx == 0:
                send(piece.at[c], own.at[c, rows(mine), :], g_send, g_recv.at[mine, c], (0, 0, dz))
            elif dz == 1:
                send(piece.at[c], stage_z.at[dx - 1, c], g_send, stage_recv.at[0, dx - 1, c], (0, 0, dz))
            else:
                send(piece.at[c], stage_x.at[dx - 1, c], g_send, stage_recv.at[1, dx - 1, c], (dx, 0, 0))

    def forward_x(dx):
        index = rank(0, 3)
        for c in range(2):
            piece = stage_z.at[dx - 1, c]
            arrived(piece, stage_recv.at[0, dx - 1, c])
            send(piece, own.at[c, rows(index), :], forward_send, g_recv.at[index, c], (dx, 0, 0))

    def forward_z(dx):
        index = rank(-dx, 0)
        for c in range(2):
            piece = stage_x.at[dx - 1, c]
            arrived(piece, stage_recv.at[1, dx - 1, c])
            send(piece, own.at[c, rows(index), :], forward_send, g_recv.at[index, c], (0, 0, 3))

    def send_weights(dz, d):
        kept = (z + dz) % SIDE // 2
        columns = columns_of(d, -dz % SIDE, z // 2)

        @brings
        def to_neighbour():
            for c in range(2):
                send(
                    weights_here.at[c, kept, d, :, columns],
                    stage_w.at[-dz % SIDE // 2, c] if d == 2 else mix.at[c, d, rows(mine), columns],
                    wz_send,
                    wz_recv.at[-dz % SIDE // 2, d, c],
                    (0, 0, dz),
                )

    def columns_of(d, dz, zs):
        return at_multiple(zs, HALF, HALF) if d == 0 and dz == 3 else slice(None)

    def mix_at(index, d, dz, c):
        return mix.at[c, d, rows(index), columns_of(d, dz, (z + dz) % SIDE // 2)]

    def to_twin(piece, d, dz):
        send(piece, piece, wt_send.at[d], wt_recv.at[dz // 2, d], (0, 0, 0, 1))

    def green_piece(dx, dz):
        index = rank(dx, dz)
        other = at_multiple((y + 1) % SIDE // 2, HALF, HALF)
        for c in range(2):
            piece = own.at[c, rows(index), :]
            arrived(piece, g_recv.at[index, c])
            send(piece, near.at[c, rows(index), :], near_send, near_recv.at[dz // 2], (0, 3, 0))
            send(own.at[c, rows(index), other], far.at[c, rows(index), :], far_send, far_recv, (0, 1, 0))

    def spread_weights(piece, d, dz, c):
        for dx in (1, 3):
            send(piece, piece, wx_send, wx_recv.at[SIDE - dx - 1, dz // 2, d, c], (dx, 0, 0))
        to_twin(piece, d, dz)

    def weights_along_z(d, dz):
        @brings
        def onward():
            for c in range(2):
                piece = mix_at(rank(0, dz), d, dz, c)
                if d == 2:
                    arrived(stage_w.at[dz // 2, c], wz_recv.at[dz // 2, d, c])
                    send(stage_w.at[dz // 2, c], piece, wy_send, wy_recv.at[dz // 2, c], (0, 1, 0))
                else:
                    arrived(piece, wz_recv.at[dz // 2, d, c])
                    spread_weights(piece, d, dz, c)

    def weights_along_y(dz):
        @brings
        def onward():
            for c in range(2):
                piece = mix_at(rank(0, dz), 2, dz, c)
                arrived(piece, wy_recv.at[dz // 2, c])
                spread_weights(piece, 2, dz, c)

    def weights_along_x(d, dz):
        @brings
        def onward():
            for c in range(2):
                for k, dx in enumerate((1, 3)):
                    piece = mix_at(rank(dx, dz), d, dz, c)
                    arrived(piece, wx_recv.at[dx - 1, dz // 2, d, c])
                    if dz // 2 == k:
                        send(piece, piece, wx_send, wx_recv.at[1, dz // 2, d, c], (-dx % SIDE, 0, 0))
                    to_twin(piece, d, dz)

    def weights_across(d, dz):
        @brings
        def hand_over():
            for c in range(2):
                piece = mix_at(rank(2, dz), d, dz, c)
                arrived(piece, wx_recv.at[1, dz // 2, d, c])
                to_twin(piece, d, dz)

    def weights_from_twin(d, dz):
        @pl.when(core == 0)
        def take():
            columns = columns_of(d, dz, (z + dz) % SIDE // 2)
            arrived(mix.at[:, d, : SIDE * RUN, columns], wt_recv.at[dz // 2, d])

    total[...] = jnp.zeros_like(total)

    def add_block(d, dz, dj, firsts, at_firsts, others, at_others, columns, weight):
        part = half(dz)

        def product(at_j):
            wr, wi = mix[0, d, part, at_j], mix[1, d, part, at_j]
            gr, gi = others[0, at_j, at_others], others[1, at_j, at_others]

            def dot(a, b):
                return jnp.dot(a, b, preferred_element_type=jnp.float32)

            return dot(wr, gr) - dot(wi, gi), dot(wr, gi) + dot(wi, gr)

        if d:
            re, im = product(half(dj))
        else:
            re, im = product(half(dz))
            if dz == 1:
                re2, im2 = product(half(3))
                re, im = re + 2.0 * re2, im + 2.0 * im2
        a = firsts[0, part, at_firsts].astype(jnp.float32)
        b = firsts[1, part, at_firsts].astype(jnp.float32)
        partial = jnp.sum((a * re + b * im).reshape(HALF // 8, 8, HALF), axis=0)
        total[:, columns] += weight * partial

    def add_own(dz):
        weights_from_twin(0, dz)
        for n in range(0, POINTS, HALF):
            span = slice(n, n + HALF)
            add_block(0, dz, None, own, span, own, span, span, 1.0)

    def add_near(dz, dj):
        for n in range(0, POINTS, HALF):
            span = slice(n, n + HALF)
            add_block(1, dz, dj, own, span, near, span, span, 2.0)

    def add_far(dz, dj):
        at_points = at_multiple(y // 2, HALF, HALF)
        add_block(2, dz, dj, far, slice(None), near, at_points, at_points, 2.0)

    for dz in (1, 3):
        send_greens(0, dz)
    for dx in (1, 3, 2):
        send_greens(dx, 3)

    @brings
    def weights_loaded():
        pltpu.make_async_copy(weights_here, weights_here, load.at[len(OUTGOING)]).wait()

    send_weights(3, 0)
    send_greens(1, 1)
    send_weights(1, 2)
    send_greens(3, 1)
    send_weights(1, 0)
    send_weights(1, 1)
    send_greens(2, 1)
    send_weights(3, 2)
    send_weights(3, 1)
    green_piece(0, 1)
    green_piece(0, 3)
    pl.semaphore_signal(met, inc=1, device_id=device(here, 0, 3), device_id_type=MESH)
    forward_z(1)
    forward_z(3)
    weights_along_z(0, 1)
    forward_x(1)
    weights_along_z(2, 1)
    weights_along_z(1, 1)
    forward_z(2)
    forward_x(3)
    green_piece(3, 1)
    weights_along_x(0, 1)
    weights_along_y(1)
    weights_along_z(0, 3)
    green_piece(3, 3)
    weights_along_z(2, 3)
    weights_along_x(1, 1)
    weights_across(0, 1)
    weights_along_z(1, 3)
    green_piece(1, 1)
    weights_along_x(2, 1)
    forward_x(2)
    green_piece(1, 3)
    weights_along_y(3)
    weights_along_x(0, 3)
    weights_across(1, 1)
    green_piece(2, 1)
    weights_across(2, 1)
    weights_along_x(1, 3)
    weights_across(0, 3)
    pl.semaphore_wait(met, 1)
    green_piece(2, 3)
    weights_along_x(2, 3)
    weights_across(1, 3)
    add_own(1)
    add_own(3)
    weights_from_twin(1, 1)
    weights_from_twin(1, 3)
    arrived(near.at[:, half(1), :], near_recv.at[0])
    add_near(1, 1)
    add_near(3, 1)
    weights_from_twin(2, 1)
    arrived(far, far_recv)
    add_far(1, 1)
    arrived(near.at[:, half(3), :], near_recv.at[1])
    add_near(1, 3)
    add_near(3, 3)
    add_far(1, 3)
    weights_across(2, 3)
    weights_from_twin(2, 3)
    add_far(3, 1)
    add_far(3, 3)

    place_in_plane = z * SIDE + y
    stations = 2 * SIDE * SIDE * RUN
    parts[place_in_plane] = jnp.sum(total[...], axis=0, keepdims=True) / stations
    for step in PLANE:
        mine_part = parts.at[place_in_plane]
        send(mine_part, mine_part, sum_send, sum_recv, step)
    arrived(parts.at[: len(PLANE)], sum_recv)
    raw = parts[0]
    for slot in range(1, SIDE * SIDE):
        raw = raw + parts[slot]
    place_in_row = core * SIDE + x
    sums[place_in_row] = raw
    for step in ROW:
        mine_sum = sums.at[place_in_row]
        send(mine_sum, mine_sum, row_send, row_recv, step)
    arrived(sums.at[: len(ROW)], row_recv)
    largest = jnp.max(jnp.abs(sums[...]))
    for k in range(SIDE):
        out[k] = sums[core * SIDE + k] / (largest + 1e-06)
    left(own, g_send)
    left(own.at[:, : 6 * RUN, :], forward_send)
    left(own, near_send)
    left(far, far_send)
    left(parts.at[: len(PLANE)], sum_send)
    left(sums.at[: len(ROW)], row_send)

    @brings
    def weights_left():
        left(mix.at[:, 0, : 11 * RUN // 2, :], wz_send)
        left(mix.at[:, :, : 11 * RUN // 2, :], wx_send)
        left(mix.at[:, 0, : 6 * RUN, :], wt_send.at[0])
        left(mix.at[:, 1], wt_send.at[1])
        left(mix.at[:, 2], wt_send.at[2])
        left(mix.at[:, 0, : 2 * RUN, :], wy_send)


def body(greens, noise_weights):
    dma = pltpu.SemaphoreType.DMA
    spread = len(SPREAD)
    ranks = 2 * SIDE
    kernel_of_points = pl.pallas_call(
        kernel,
        out_shape=jax.ShapeDtypeStruct((SIDE, 1, POINTS), jnp.float32),
        in_specs=[pl.BlockSpec(memory_space=pl.ANY)] * 2,
        out_specs=pl.BlockSpec(memory_space=pltpu.VMEM),
        scratch_shapes=[
            pltpu.VMEM((2, BLOCK, POINTS), jnp.bfloat16),
            pltpu.VMEM((2, BLOCK, POINTS), jnp.bfloat16),
            pltpu.VMEM((2, BLOCK, HALF), jnp.bfloat16),
            pltpu.VMEM((2, 2, RUN, BLOCK), jnp.bfloat16),
            pltpu.VMEM((2, 3, BLOCK, BLOCK), jnp.bfloat16),
            pltpu.VMEM((SIDE * SIDE, 1, POINTS), jnp.float32),
            pltpu.VMEM((8, POINTS), jnp.float32),
            pltpu.VMEM((ranks, 1, POINTS), jnp.float32),
            dma,
            dma((ranks, 2)),
            dma,
            dma((2,)),
            dma,
            dma((2, 2)),
            dma,
            dma,
            dma,
            dma((2, 3, 2)),
            dma,
            dma((3, 2, 3, 2)),
            dma((3,)),
            dma((2, 3)),
            dma,
            dma,
            dma,
            dma,
            pltpu.VMEM((spread, 2, RUN, POINTS), jnp.bfloat16),
            pltpu.VMEM((2, 2, 3, RUN, BLOCK), jnp.bfloat16),
            dma((spread + 1,)),
            pltpu.VMEM((3, 2, RUN, POINTS), jnp.bfloat16),
            pltpu.VMEM((3, 2, RUN, POINTS), jnp.bfloat16),
            dma((2, 3, 2)),
            dma,
            pltpu.SemaphoreType.REGULAR,
        ],
        compiler_params=pltpu.CompilerParams(
            collective_id=0, has_side_effects=True, vmem_limit_bytes=213 * 2**18
        ),
    )(greens, noise_weights)
    return kernel_of_points.reshape(SIDE * POINTS)


def solution(mesh):
    in_specs = (P(None, "freq", "stn", "pts"), P(None, "freq", "stn", None))
    out_specs = P("pts")
    return jax.shard_map(body, mesh=mesh, in_specs=in_specs, out_specs=out_specs, check_vma=False)
```

```python
import jax
import jax.numpy as jnp
from jax import lax
from jax.experimental import pallas as pl
from jax.experimental.pallas import tpu as pltpu
from jax.sharding import PartitionSpec as P

MESH = pl.DeviceIdType.MESH
SIDE = 4
RUN = 64
BLOCK = 512
POINTS = 512
HALF = 256

SPREAD = [(dx, 0, dz, 0) for dx in (0, 1, 3, 2) for dz in (1, 3)]
PLANE = [(0, dy, dz, 0) for dz in range(SIDE) for dy in range(SIDE) if dy or dz]
ROW = [(dx, 0, 0, dc) for dx in range(SIDE) for dc in range(2) if dx or dc]
OUTGOING = [(0, 1), (0, 3), (1, 3), (3, 3), (1, 1), (3, 1), (2, 3), (2, 1)]
NEAREST = [(1, 0, 0), (3, 0, 0), (2, 0, 0), (0, 1, 0), (0, 3, 0), (0, 0, 1), (0, 0, 3), (0, 0, 0, 1)]


def place():
    stn = lax.axis_index("stn")
    x, y = stn % SIDE, stn // SIDE % SIDE
    z = stn // (SIDE * SIDE) * 2 + lax.axis_index("freq")
    return x, y, z, lax.axis_index("pts")


def device(here, dx=0, dy=0, dz=0, dc=0):
    x, y, z, core = here
    x, y, z, core = (x + dx) % SIDE, (y + dy) % SIDE, (z + dz) % SIDE, (core + dc) % 2
    return {"stn": z // 2 * (SIDE * SIDE) + y * SIDE + x, "freq": z % 2, "pts": core}


def at_multiple(index, size, length):
    return pl.ds(pl.multiple_of(index * size, size), length)


def kernel(
    greens,
    weights,
    out,
    own,
    near,
    far,
    stage_w,
    mix,
    parts,
    total,
    sums,
    g_send,
    g_recv,
    near_send,
    near_recv,
    wy_send,
    wy_recv,
    far_send,
    far_recv,
    wz_send,
    wz_recv,
    wx_send,
    wx_recv,
    wt_send,
    wt_recv,
    sum_send,
    sum_recv,
    row_send,
    row_recv,
    greens_here,
    weights_here,
    load,
    stage_x,
    stage_z,
    stage_recv,
    forward_send,
    met,
):
    here = place()
    x, y, z, core = here

    barrier = pltpu.get_barrier_semaphore()
    for step in NEAREST:
        pl.semaphore_signal(barrier, inc=1, device_id=device(here, *step), device_id_type=MESH)

    def at_greens(dx, dz):
        columns = at_multiple((x + dx) % SIDE, POINTS, POINTS)
        return slice(None), (z + dz) % SIDE // 2, slice(None), columns

    greens_in = {}
    for k, (dx, dz) in enumerate(OUTGOING):
        part = at_greens(dx, dz)
        greens_in[dx, dz] = pltpu.make_async_copy(greens.at[part], greens_here.at[k], load.at[k])
        greens_in[dx, dz].start()

    brings = pl.when(core == 1)

    @brings
    def load_weights():
        for d in range(3):
            for zs in range(2):
                columns = at_multiple(zs * SIDE + (y + d) % SIDE, HALF, HALF)
                pltpu.make_async_copy(
                    weights.at[:, :, :, columns],
                    weights_here.at[:, :, d, :, zs * HALF : (zs + 1) * HALF],
                    load.at[len(OUTGOING)],
                ).start()

    pl.semaphore_wait(barrier, len(NEAREST))

    def send(src, dst, send_sem, recv_sem, step):
        copy = pltpu.make_async_remote_copy(
            src_ref=src,
            dst_ref=dst,
            send_sem=send_sem,
            recv_sem=recv_sem,
            device_id=device(here, *step),
            device_id_type=MESH,
        )
        copy.start()

    def arrived(dst, sem):
        pltpu.make_async_remote_copy(
            src_ref=dst,
            dst_ref=dst,
            send_sem=sem,
            recv_sem=sem,
            device_id=device(here, 1),
            device_id_type=MESH,
        ).wait_recv()

    def left(src, sem):
        pltpu.make_async_remote_copy(
            src_ref=src,
            dst_ref=src,
            send_sem=sem,
            recv_sem=sem,
            device_id=device(here, 1),
            device_id_type=MESH,
        ).wait_send()

    def rank(dx, dz):
        return (z + dz) % SIDE // 2 * SIDE + (x + dx) % SIDE

    def rows(index):
        return at_multiple(index, RUN, RUN)

    mine = rank(0, 0)

    def half(dz):
        return at_multiple((z + dz) % SIDE // 2, HALF, HALF)

    def send_greens(dx, dz):
        piece = greens_here.at[OUTGOING.index((dx, dz))]
        greens_in[dx, dz].wait()
        for c in range(2):
            if dx == 0:
                send(piece.at[c], own.at[c, rows(mine), :], g_send, g_recv.at[mine, c], (0, 0, dz))
            elif dz == 1:
                send(piece.at[c], stage_z.at[dx - 1, c], g_send, stage_recv.at[0, dx - 1, c], (0, 0, dz))
            else:
                send(piece.at[c], stage_x.at[dx - 1, c], g_send, stage_recv.at[1, dx - 1, c], (dx, 0, 0))

    def forward_x(dx):
        index = rank(0, 3)
        for c in range(2):
            piece = stage_z.at[dx - 1, c]
            arrived(piece, stage_recv.at[0, dx - 1, c])
            send(piece, own.at[c, rows(index), :], forward_send, g_recv.at[index, c], (dx, 0, 0))

    def forward_z(dx):
        index = rank(-dx, 0)
        for c in range(2):
            piece = stage_x.at[dx - 1, c]
            arrived(piece, stage_recv.at[1, dx - 1, c])
            send(piece, own.at[c, rows(index), :], forward_send, g_recv.at[index, c], (0, 0, 3))

    def send_weights(dz, d):
        kept = (z + dz) % SIDE // 2
        columns = columns_of(d, -dz % SIDE, z // 2)

        @brings
        def to_neighbour():
            for c in range(2):
                send(
                    weights_here.at[c, kept, d, :, columns],
                    stage_w.at[-dz % SIDE // 2, c] if d == 2 else mix.at[c, d, rows(mine), columns],
                    wz_send,
                    wz_recv.at[-dz % SIDE // 2, d, c],
                    (0, 0, dz),
                )

    def columns_of(d, dz, zs):
        return at_multiple(zs, HALF, HALF) if d == 0 and dz == 3 else slice(None)

    def mix_at(index, d, dz, c):
        return mix.at[c, d, rows(index), columns_of(d, dz, (z + dz) % SIDE // 2)]

    def to_twin(piece, d, dz):
        send(piece, piece, wt_send.at[d], wt_recv.at[dz // 2, d], (0, 0, 0, 1))

    def green_piece(dx, dz):
        index = rank(dx, dz)
        other = at_multiple((y + 1) % SIDE // 2, HALF, HALF)
        for c in range(2):
            piece = own.at[c, rows(index), :]
            arrived(piece, g_recv.at[index, c])
            send(piece, near.at[c, rows(index), :], near_send, near_recv.at[dz // 2], (0, 3, 0))
            send(own.at[c, rows(index), other], far.at[c, rows(index), :], far_send, far_recv, (0, 1, 0))

    def spread_weights(piece, d, dz, c):
        for dx in (1, 3):
            send(piece, piece, wx_send, wx_recv.at[SIDE - dx - 1, dz // 2, d, c], (dx, 0, 0))
        to_twin(piece, d, dz)

    def weights_along_z(d, dz):
        @brings
        def onward():
            for c in range(2):
                piece = mix_at(rank(0, dz), d, dz, c)
                if d == 2:
                    arrived(stage_w.at[dz // 2, c], wz_recv.at[dz // 2, d, c])
                    send(stage_w.at[dz // 2, c], piece, wy_send, wy_recv.at[dz // 2, c], (0, 1, 0))
                else:
                    arrived(piece, wz_recv.at[dz // 2, d, c])
                    spread_weights(piece, d, dz, c)

    def weights_along_y(dz):
        @brings
        def onward():
            for c in range(2):
                piece = mix_at(rank(0, dz), 2, dz, c)
                arrived(piece, wy_recv.at[dz // 2, c])
                spread_weights(piece, 2, dz, c)

    def weights_along_x(d, dz):
        @brings
        def onward():
            for c in range(2):
                for k, dx in enumerate((1, 3)):
                    piece = mix_at(rank(dx, dz), d, dz, c)
                    arrived(piece, wx_recv.at[dx - 1, dz // 2, d, c])
                    if dz // 2 == k:
                        send(piece, piece, wx_send, wx_recv.at[1, dz // 2, d, c], (-dx % SIDE, 0, 0))
                    to_twin(piece, d, dz)

    def weights_across(d, dz):
        @brings
        def hand_over():
            for c in range(2):
                piece = mix_at(rank(2, dz), d, dz, c)
                arrived(piece, wx_recv.at[1, dz // 2, d, c])
                to_twin(piece, d, dz)

    def weights_from_twin(d, dz):
        @pl.when(core == 0)
        def take():
            columns = columns_of(d, dz, (z + dz) % SIDE // 2)
            arrived(mix.at[:, d, : SIDE * RUN, columns], wt_recv.at[dz // 2, d])

    total[...] = jnp.zeros_like(total)

    def add_block(d, dz, dj, firsts, at_firsts, others, at_others, columns, weight):
        part = half(dz)

        def product(at_j):
            wr, wi = mix[0, d, part, at_j], mix[1, d, part, at_j]
            gr, gi = others[0, at_j, at_others], others[1, at_j, at_others]

            def dot(a, b):
                return jnp.dot(a, b, preferred_element_type=jnp.float32)

            return dot(wr, gr) - dot(wi, gi), dot(wr, gi) + dot(wi, gr)

        if d:
            re, im = product(half(dj))
        else:
            re, im = product(half(dz))
            if dz == 1:
                re2, im2 = product(half(3))
                re, im = re + 2.0 * re2, im + 2.0 * im2
        a = firsts[0, part, at_firsts].astype(jnp.float32)
        b = firsts[1, part, at_firsts].astype(jnp.float32)
        partial = jnp.sum((a * re + b * im).reshape(HALF // 8, 8, HALF), axis=0)
        total[:, columns] += weight * partial

    def add_own(dz):
        weights_from_twin(0, dz)
        for n in range(0, POINTS, HALF):
            span = slice(n, n + HALF)
            add_block(0, dz, None, own, span, own, span, span, 1.0)

    def add_near(dz, dj):
        for n in range(0, POINTS, HALF):
            span = slice(n, n + HALF)
            add_block(1, dz, dj, own, span, near, span, span, 2.0)

    def add_far(dz, dj):
        at_points = at_multiple(y // 2, HALF, HALF)
        add_block(2, dz, dj, far, slice(None), near, at_points, at_points, 2.0)

    for dz in (1, 3):
        send_greens(0, dz)
    for dx in (1, 3, 2):
        send_greens(dx, 3)

    @brings
    def weights_loaded():
        pltpu.make_async_copy(weights_here, weights_here, load.at[len(OUTGOING)]).wait()

    send_weights(3, 0)
    send_greens(1, 1)
    send_weights(1, 2)
    send_greens(3, 1)
    send_weights(1, 0)
    send_weights(1, 1)
    send_greens(2, 1)
    send_weights(3, 2)
    send_weights(3, 1)
    green_piece(0, 1)
    green_piece(0, 3)
    pl.semaphore_signal(met, inc=1, device_id=device(here, 0, 3), device_id_type=MESH)
    forward_z(1)
    forward_z(3)
    weights_along_z(0, 1)
    forward_x(1)
    weights_along_z(2, 1)
    forward_x(3)
    forward_z(2)
    weights_along_z(1, 1)
    weights_along_x(0, 1)
    green_piece(3, 1)
    weights_along_y(1)
    weights_along_z(0, 3)
    green_piece(3, 3)
    weights_along_z(2, 3)
    weights_along_x(1, 1)
    green_piece(1, 1)
    weights_across(0, 1)
    weights_along_z(1, 3)
    weights_along_x(2, 1)
    green_piece(1, 3)
    forward_x(2)
    weights_along_x(0, 3)
    weights_along_y(3)
    weights_across(1, 1)
    green_piece(2, 1)
    weights_across(2, 1)
    weights_along_x(1, 3)
    pl.semaphore_wait(met, 1)
    green_piece(2, 3)
    weights_across(0, 3)
    weights_along_x(2, 3)
    weights_across(1, 3)
    add_own(1)
    add_own(3)
    weights_from_twin(1, 1)
    weights_from_twin(1, 3)
    arrived(near.at[:, half(1), :], near_recv.at[0])
    add_near(1, 1)
    add_near(3, 1)
    weights_from_twin(2, 1)
    arrived(far, far_recv)
    add_far(1, 1)
    arrived(near.at[:, half(3), :], near_recv.at[1])
    add_near(1, 3)
    add_near(3, 3)
    add_far(1, 3)
    weights_across(2, 3)
    weights_from_twin(2, 3)
    add_far(3, 1)
    add_far(3, 3)

    place_in_plane = z * SIDE + y
    stations = 2 * SIDE * SIDE * RUN
    parts[place_in_plane] = jnp.sum(total[...], axis=0, keepdims=True) / stations
    for step in PLANE:
        mine_part = parts.at[place_in_plane]
        send(mine_part, mine_part, sum_send, sum_recv, step)
    arrived(parts.at[: len(PLANE)], sum_recv)
    raw = parts[0]
    for slot in range(1, SIDE * SIDE):
        raw = raw + parts[slot]
    place_in_row = core * SIDE + x
    sums[place_in_row] = raw
    for step in ROW:
        mine_sum = sums.at[place_in_row]
        send(mine_sum, mine_sum, row_send, row_recv, step)
    arrived(sums.at[: len(ROW)], row_recv)
    largest = jnp.max(jnp.abs(sums[...]))
    for k in range(SIDE):
        out[k] = sums[core * SIDE + k] / (largest + 1e-06)
    left(own, g_send)
    left(own.at[:, : 6 * RUN, :], forward_send)
    left(own, near_send)
    left(far, far_send)
    left(parts.at[: len(PLANE)], sum_send)
    left(sums.at[: len(ROW)], row_send)

    @brings
    def weights_left():
        left(mix.at[:, 0, : 11 * RUN // 2, :], wz_send)
        left(mix.at[:, :, : 11 * RUN // 2, :], wx_send)
        left(mix.at[:, 0, : 6 * RUN, :], wt_send.at[0])
        left(mix.at[:, 1], wt_send.at[1])
        left(mix.at[:, 2], wt_send.at[2])
        left(mix.at[:, 0, : 2 * RUN, :], wy_send)


def body(greens, noise_weights):
    dma = pltpu.SemaphoreType.DMA
    spread = len(SPREAD)
    ranks = 2 * SIDE
    kernel_of_points = pl.pallas_call(
        kernel,
        out_shape=jax.ShapeDtypeStruct((SIDE, 1, POINTS), jnp.float32),
        in_specs=[pl.BlockSpec(memory_space=pl.ANY)] * 2,
        out_specs=pl.BlockSpec(memory_space=pltpu.VMEM),
        scratch_shapes=[
            pltpu.VMEM((2, BLOCK, POINTS), jnp.bfloat16),
            pltpu.VMEM((2, BLOCK, POINTS), jnp.bfloat16),
            pltpu.VMEM((2, BLOCK, HALF), jnp.bfloat16),
            pltpu.VMEM((2, 2, RUN, BLOCK), jnp.bfloat16),
            pltpu.VMEM((2, 3, BLOCK, BLOCK), jnp.bfloat16),
            pltpu.VMEM((SIDE * SIDE, 1, POINTS), jnp.float32),
            pltpu.VMEM((8, POINTS), jnp.float32),
            pltpu.VMEM((ranks, 1, POINTS), jnp.float32),
            dma,
            dma((ranks, 2)),
            dma,
            dma((2,)),
            dma,
            dma((2, 2)),
            dma,
            dma,
            dma,
            dma((2, 3, 2)),
            dma,
            dma((3, 2, 3, 2)),
            dma((3,)),
            dma((2, 3)),
            dma,
            dma,
            dma,
            dma,
            pltpu.VMEM((spread, 2, RUN, POINTS), jnp.bfloat16),
            pltpu.VMEM((2, 2, 3, RUN, BLOCK), jnp.bfloat16),
            dma((spread + 1,)),
            pltpu.VMEM((3, 2, RUN, POINTS), jnp.bfloat16),
            pltpu.VMEM((3, 2, RUN, POINTS), jnp.bfloat16),
            dma((2, 3, 2)),
            dma,
            pltpu.SemaphoreType.REGULAR,
        ],
        compiler_params=pltpu.CompilerParams(
            collective_id=0, has_side_effects=True, vmem_limit_bytes=213 * 2**18
        ),
    )(greens, noise_weights)
    return kernel_of_points.reshape(SIDE * POINTS)


def solution(mesh):
    in_specs = (P(None, "freq", "stn", "pts"), P(None, "freq", "stn", None))
    out_specs = P("pts")
    return jax.shard_map(body, mesh=mesh, in_specs=in_specs, out_specs=out_specs, check_vma=False)
```
